32 devices in a mesh: grp: 2 (over y), seq: 16 (over z, x, core).
Axes of the slice: x: 2, y: 2, z: 4, core: 2. Of those that a mesh axis runs over, the one named last changes fastest.
Arguments:
- queries: bfloat16 [4096, 12288], P(('grp', 'seq')), parts along dimension 0, may hold values from -8 to 8
- sum_keys: bfloat16 [256, 768], P(('grp', 'seq')), parts along dimension 0, may hold values from -4 to 4
- sum_values: bfloat16 [256, 512], P(('grp', 'seq')), parts along dimension 0, may hold values from -24 to 24
- limits: int32 [64], P('grp'), parts along dimension 0, may hold values from 1 to 128, as said below
- valid_tokens: int32 [2], P('grp'), parts along dimension 0, may hold values from 1024 to 2048
Outputs:
- attended: bfloat16 [4096, 8192], P(('grp', 'seq')), parts along dimension 0
The draws below stay inside these ranges and needn't reach their ends.
There are 2 independent parts, one for each index of `grp`. The reference program is written for one: setup_inputs(seed, part) draws one part's arguments, and reference() takes and returns one part's arrays. A program takes and returns all parts, laid end to end along the dimension named above; each array names one. Nothing has to cross between parts.
Inputs may be any that keep to these rules, and one draw needn't show every extreme that they name: limits[b] is at least 1 and at most max(1, (64 * b - 32) // 16 + 1), the number of summaries that end at or before the block's first token; the last block reaches this bound.
All inputs are finite; a program needn't handle non-finite values.
Results may differ from the reference program's by a relative error of at most 0.0027.
Values may be sent and summed in bfloat16 or wider, within the bound.
No kernel may reach another device: no remote copies, remote signals or barrier semaphores. Data moves between devices by JAX's collectives and lax.ppermute only.
A program may use at most 64 MiB of HBM per device.

```python
import jax
import jax.numpy as jnp
from jax import lax

H = 64
G = 4
DK = 192
DV = 128
STRIDE = 16
CBLOCK = 32
QB = 64
L = 2048
NS = 128
NB = 32


def summary_key_law(key):
    inner = jax.random.fold_in(key, 11)
    values = jnp.clip(jax.random.normal(inner, (NS, G * DK)), -4.0, 4.0)
    return values.astype(jnp.float32)


def draw_sum_keys(key, part):
    return summary_key_law(key).astype(jnp.bfloat16)


def draw_queries(key, part):
    inner = jax.random.fold_in(key, 23)
    values = jnp.clip(2.5 * jax.random.normal(inner, (L, H * DK)), -8.0, 8.0)
    return values.astype(jnp.bfloat16)


def draw_limits(key, part):
    block_ids = jnp.arange(NB, dtype=jnp.int32)
    causal = jnp.maximum((QB * block_ids - CBLOCK) // STRIDE + 1, 1).astype(jnp.int32)
    offsets = jax.random.randint(jax.random.fold_in(key, 5), (NB,), 0, 1 << 20, dtype=jnp.int32) % (causal // 4 + 1)
    drawn = causal - offsets
    return drawn.at[NB - 1].set(causal[NB - 1]).astype(jnp.int32)


def shard_levels(stream_key, dims, pieces, smallest, high):
    def one(dim, parts):
        heights = jax.random.uniform(jax.random.fold_in(jax.random.fold_in(stream_key, 6), dim), (parts,), jnp.float32, smallest / len(pieces), high / len(pieces))
        return jnp.repeat(jnp.exp(heights), dims[dim] // parts).reshape((-1,) + (1,) * (len(dims) - dim - 1))

    loudness = one(*pieces[0])
    for cut in pieces[1:]:
        loudness = loudness * one(*cut)
    return loudness


def scatter_about(own_key, extent, scale, most, cuts=(), kind=jnp.bfloat16):
    gain = shard_levels(own_key, extent, cuts, -0.22, 0.18) if cuts else 1.0
    result = jax.random.normal(own_key, extent, jnp.float32) * scale * gain
    return jnp.minimum(jnp.maximum(result, -most), most).astype(kind)


def setup_inputs(seed: int = 0, part: int = 0) -> dict:
    splits = jax.random.split(jax.random.key(seed), 6)
    part_splits = jax.random.split(jax.random.fold_in(splits[5], part), 6)
    return {
        "queries": draw_queries(jax.random.fold_in(jax.random.fold_in(splits[5], part), 71), part),
        "sum_keys": draw_sum_keys(jax.random.fold_in(jax.random.fold_in(splits[5], part), 71), part),
        "sum_values": scatter_about(part_splits[2], (NS, G * DV), 4.0, 24.0, ((0, 16),)),
        "limits": draw_limits(jax.random.fold_in(jax.random.fold_in(splits[5], part), 71), part),
        "valid_tokens": jax.random.randint(part_splits[4], (1,), L // 2, L + 1).astype(jnp.int32),
    }


def reference(queries, sum_keys, sum_values, limits, valid_tokens):
    per_group = H // G
    inv_root = float(DK) ** -0.5
    usable = jnp.maximum((valid_tokens[0] - CBLOCK) // STRIDE + 1, 1).astype(jnp.int32)
    key_table = sum_keys.reshape(NS, G, DK).astype(jnp.float32)
    value_table = sum_values.reshape(NS, G, DV).astype(jnp.float32)
    summary_ids = jnp.arange(NS, dtype=jnp.int32)

    def one_block(block_args):
        query_block, block_limit = block_args
        grouped = query_block.reshape(QB, G, per_group, DK).astype(jnp.float32)
        scores = jnp.einsum("tgjd,sgd->tgjs", grouped, key_table, precision=lax.Precision.HIGHEST) * inv_root
        visible = summary_ids < jnp.minimum(block_limit, usable)
        scores = jnp.where(visible, scores, -1e30)
        row_max = jnp.max(scores, axis=-1, keepdims=True)
        weights = jnp.where(visible, jnp.exp(scores - row_max), 0.0)
        row_total = jnp.sum(weights, axis=-1, keepdims=True)
        rounded = lax.optimization_barrier(weights.astype(jnp.bfloat16)).astype(jnp.float32)
        blended = jnp.einsum("tgjs,sgd->tgjd", rounded, value_table, precision=lax.Precision.HIGHEST) / row_total
        return blended.reshape(QB, H * DV).astype(jnp.bfloat16)

    blocks = lax.map(one_block, (queries.reshape(NB, QB, H * DK), limits))
    return blocks.reshape(L, H * DV)
```

```python
import functools
import math

import jax
import jax.numpy as jnp
from jax import lax
from jax.experimental import pallas as pl
from jax.experimental.pallas import tpu as pltpu
from jax.sharding import PartitionSpec as P

H = 64
G = 4
DK = 192
DV = 128
STRIDE = 16
CBLOCK = 32
QB = 64
PER = H // G
HIDDEN = -1e30


def exchange_masks(count):
    bits = count.bit_length() - 1
    return [(1 << b) | 1 for b in range(bits - 1, 0, -1)] + [1]


def gather_parts(x, count):
    if count < 2 or count & (count - 1) or x.shape[0] & (x.shape[0] - 1):
        whole = lax.all_gather(x, "seq", axis=0, tiled=True)
        return [whole], None
    masks = exchange_masks(count)
    for mask in masks[:-1]:
        other = lax.ppermute(x, "seq", [(i, i ^ mask) for i in range(count)])
        x = jnp.concatenate([x, other], axis=0)
    other = lax.ppermute(x, "seq", [(i, i ^ masks[-1]) for i in range(count)])
    return [x, other], masks


def attend(masks, shard, parts, *refs):
    q_ref, *kv_refs = refs[: 1 + parts]
    limits_ref, valid_ref, out_ref, o_ref, sem = refs[1 + parts :]
    tokens = q_ref.shape[0]
    total = sum(r.shape[0] for r in kv_refs)
    blocks = tokens // QB
    me = lax.axis_index("seq")
    usable = jnp.maximum(((valid_ref[0] - CBLOCK) >> (STRIDE.bit_length() - 1)) + 1, 1)
    lane = lax.broadcasted_iota(jnp.int32, (8, total), 1)
    if masks is None:
        ids = lane
    else:
        low = shard.bit_length() - 1
        owner = jnp.full_like(lane, me)
        for bit, mask in enumerate(masks):
            owner = owner ^ (((lane >> (low + bit)) & 1) * mask)
        ids = owner * shard + (lane & (shard - 1))
    biases = [
        jnp.where(ids < jnp.minimum(limits_ref[me * blocks + b], usable), 0.0, HIDDEN)[:1]
        for b in range(blocks)
    ]
    factor = math.log2(math.e) * float(DK) ** -0.5
    wide = 2 * DV
    col = lax.broadcasted_iota(jnp.int32, (total, wide), 1)

    def keys_at(g, offset):
        start = g * DK
        base = start // 128 * 128
        window = jnp.concatenate([r[:, base : base + wide] for r in kv_refs], axis=0).astype(jnp.float32)
        shift = (offset - (start - base)) % wide
        if shift:
            window = pltpu.roll(window, shift, 1)
        return jnp.where((col >= offset) & (col < offset + DK), window, 0.0).astype(jnp.bfloat16)

    pairs = PER // 2
    copies = []
    for g in range(G):
        v_start = G * DK + g * DV
        values = jnp.concatenate([r[:, v_start : v_start + DV] for r in kv_refs], axis=0)
        sides = []
        for side in range(2):
            weights = keys_at(g, side * (wide - DK))
            q0 = g * PER * DK + side * 128
            rows = jnp.concatenate(
                [q_ref[:, q0 + j * 2 * DK : q0 + j * 2 * DK + wide] for j in range(pairs)], axis=0
            )
            scores = lax.dot_general(
                rows, weights, (((1,), (1,)), ((), ())), preferred_element_type=jnp.float32
            )
            scores = scores.reshape(pairs, blocks, QB, total)
            scores = jnp.concatenate([scores[:, b : b + 1] + biases[b] for b in range(blocks)], axis=1)
            scores = scores.reshape(pairs * tokens, total)
            top = jnp.max(scores, axis=1, keepdims=True)
            w = jnp.exp2((scores - top) * factor)
            norm = jnp.sum(w, axis=1, keepdims=True)
            sides.append((w.astype(jnp.bfloat16), 1.0 / norm))
        (wa, ra), (wb, rb) = sides
        if total <= 128:
            zeros = jnp.zeros_like(values)
            both = jnp.concatenate(
                [jnp.concatenate([values, zeros], axis=1), jnp.concatenate([zeros, values], axis=1)], axis=0
            )
            out = jnp.dot(jnp.concatenate([wa, wb], axis=1), both, preferred_element_type=jnp.float32)
            outa, outb = out[:, :DV], out[:, DV:]
        else:
            outa = jnp.dot(wa, values, preferred_element_type=jnp.float32)
            outb = jnp.dot(wb, values, preferred_element_type=jnp.float32)
        outa = (outa * ra).astype(jnp.bfloat16)
        outb = (outb * rb).astype(jnp.bfloat16)
        for j in range(pairs):
            at = (g * PER + 2 * j) * DV
            o_ref[:, at : at + DV] = outa[j * tokens : (j + 1) * tokens]
            o_ref[:, at + DV : at + 2 * DV] = outb[j * tokens : (j + 1) * tokens]
        span = pl.ds(g * PER * DV, PER * DV)
        copy = pltpu.make_async_copy(o_ref.at[:, span], out_ref.at[:, span], sem.at[g])
        copy.start()
        copies.append(copy)
    for copy in copies:
        copy.wait()


def per_device(count, queries, sum_keys, sum_values, limits, valid_tokens):
    tokens = queries.shape[0]
    shard = sum_keys.shape[0]
    halves, masks = gather_parts(jnp.concatenate([sum_keys, sum_values], axis=1), count)
    vmem = pl.BlockSpec(memory_space=pltpu.VMEM)
    smem = pl.BlockSpec(memory_space=pltpu.SMEM)
    return pl.pallas_call(
        functools.partial(attend, masks, shard, len(halves)),
        out_shape=jax.ShapeDtypeStruct((tokens, H * DV), jnp.bfloat16),
        in_specs=[vmem] * (1 + len(halves)) + [smem, smem],
        out_specs=pl.BlockSpec(memory_space=pl.ANY),
        scratch_shapes=[pltpu.VMEM((tokens, H * DV), jnp.bfloat16), pltpu.SemaphoreType.DMA((G,))],
        compiler_params=pltpu.CompilerParams(vmem_limit_bytes=40 * 1024 * 1024),
    )(queries, *halves, limits, valid_tokens)


def solution(mesh):
    placed = (
        P(("grp", "seq"), None),
        P(("grp", "seq"), None),
        P(("grp", "seq"), None),
        P("grp"),
        P("grp"),
    )
    return jax.shard_map(
        functools.partial(per_device, mesh.shape["seq"]),
        mesh=mesh,
        in_specs=placed,
        out_specs=P(("grp", "seq"), None),
        check_vma=False,
    )
```

```python
import functools
import math

import jax
import jax.numpy as jnp
from jax import lax
from jax.experimental import pallas as pl
from jax.experimental.pallas import tpu as pltpu
from jax.sharding import PartitionSpec as P


H = 64
G = 4
DK = 192
DV = 128
STRIDE = 16
CBLOCK = 32
QB = 64
PER = H // G
HIDDEN = -1e30
STAGE_BYTES = 1024 * 1024


def exchange_masks(count):
    bits = count.bit_length() - 1
    return [(1 << b) | 1 for b in range(bits - 1, 0, -1)] + [1]


def gather_parts(x, count):
    if count < 2 or count & (count - 1) or x.shape[0] & (x.shape[0] - 1):
        whole = lax.all_gather(x, "seq", axis=0, tiled=True)
        return [whole], None
    masks = exchange_masks(count)
    for bit, mask in enumerate(masks):
        other = lax.ppermute(x, "seq", [(i, i ^ mask) for i in range(count)])
        if bit < len(masks) - 1:
            x = jnp.concatenate([x, other], axis=0)
    return [x, other], masks


def stage(masks, shard, limits_ref, valid_ref, bias_ref):
    blocks, total = bias_ref.shape[0] // 8, bias_ref.shape[1]
    me = lax.axis_index("seq")
    usable = jnp.maximum(((valid_ref[0] - CBLOCK) >> (STRIDE.bit_length() - 1)) + 1, 1)
    lane = lax.broadcasted_iota(jnp.int32, (8, total), 1)
    if masks is None:
        ids = lane
    else:
        low = shard.bit_length() - 1
        owner = jnp.full_like(lane, me)
        for bit, mask in enumerate(masks):
            owner = owner ^ (((lane >> (low + bit)) & 1) * mask)
        ids = owner * shard + (lane & (shard - 1))
    for b in range(blocks):
        cap = jnp.minimum(limits_ref[me * blocks + b], usable)
        bias_ref[8 * b : 8 * b + 8] = jnp.where(ids < cap, 0.0, HIDDEN)


def attend(parts, *refs):
    q_ref, bias_ref, *kv_refs = refs[: 2 + parts]
    out_ref, o_ref, sem = refs[2 + parts :]
    tokens = q_ref.shape[0]
    total = sum(r.shape[0] for r in kv_refs)
    blocks = tokens // QB
    biases = [bias_ref[8 * b : 8 * b + 1] for b in range(blocks)]
    factor = math.log2(math.e) * float(DK) ** -0.5
    wide = 2 * DV
    col = lax.broadcasted_iota(jnp.int32, (total, wide), 1)

    def keys_at(g, offset):
        start = g * DK
        base = start // 128 * 128
        window = jnp.concatenate([r[:, base : base + wide] for r in kv_refs], axis=0).astype(jnp.float32)
        shift = (offset - (start - base)) % wide
        if shift:
            window = pltpu.roll(window, shift, 1)
        return jnp.where((col >= offset) & (col < offset + DK), window, 0.0).astype(jnp.bfloat16)

    pairs = PER // 2
    copies = []
    for g in range(G):
        v_start = G * DK + g * DV
        values = jnp.concatenate([r[:, v_start : v_start + DV] for r in kv_refs], axis=0)
        sides = []
        for side in range(2):
            weights = keys_at(g, side * (wide - DK))
            q0 = g * PER * DK + side * 128
            rows = jnp.concatenate(
                [q_ref[:, q0 + j * 2 * DK : q0 + j * 2 * DK + wide] for j in range(pairs)], axis=0
            )
            scores = lax.dot_general(
                rows, weights, (((1,), (1,)), ((), ())), preferred_element_type=jnp.float32
            )
            scores = scores.reshape(pairs, blocks, QB, total)
            scores = jnp.concatenate([scores[:, b : b + 1] + biases[b] for b in range(blocks)], axis=1)
            scores = scores.reshape(pairs * tokens, total)
            top = jnp.max(scores, axis=1, keepdims=True)
            w = jnp.exp2((scores - top) * factor)
            norm = jnp.sum(w, axis=1, keepdims=True)
            sides.append((w.astype(jnp.bfloat16), 1.0 / norm))
        (wa, ra), (wb, rb) = sides
        if total <= 128:
            zeros = jnp.zeros_like(values)
            both = jnp.concatenate(
                [jnp.concatenate([values, zeros], axis=1), jnp.concatenate([zeros, values], axis=1)], axis=0
            )
            out = jnp.dot(jnp.concatenate([wa, wb], axis=1), both, preferred_element_type=jnp.float32)
            outa, outb = out[:, :DV], out[:, DV:]
        else:
            outa = jnp.dot(wa, values, preferred_element_type=jnp.float32)
            outb = jnp.dot(wb, values, preferred_element_type=jnp.float32)
        outa = (outa * ra).astype(jnp.bfloat16)
        outb = (outb * rb).astype(jnp.bfloat16)
        for j in range(pairs):
            at = (g * PER + 2 * j) * DV
            o_ref[:, at : at + DV] = outa[j * tokens : (j + 1) * tokens]
            o_ref[:, at + DV : at + 2 * DV] = outb[j * tokens : (j + 1) * tokens]
        span = pl.ds(g * PER * DV, PER * DV)
        copy = pltpu.make_async_copy(o_ref.at[:, span], out_ref.at[:, span], sem.at[g])
        copy.start()
        copies.append(copy)
    for copy in copies:
        copy.wait()


def layer(count, queries, sum_keys, sum_values, limits, valid_tokens):
    tokens = queries.shape[0]
    shard = sum_keys.shape[0]
    vmem = pl.BlockSpec(memory_space=pltpu.VMEM)
    smem = pl.BlockSpec(memory_space=pltpu.SMEM)
    hbm = pl.BlockSpec(memory_space=pl.ANY)
    low = jnp.array(-jnp.inf, sum_keys.dtype)
    packed = jnp.maximum(
        lax.pad(sum_keys, low, ((0, 0, 0), (0, sum_values.shape[1], 0))),
        lax.pad(sum_values, low, ((0, 0, 0), (sum_keys.shape[1], 0, 0))),
    )
    halves, masks = gather_parts(packed, count)
    biases = pl.pallas_call(
        functools.partial(stage, masks, shard),
        out_shape=jax.ShapeDtypeStruct((tokens // QB * 8, shard * count), jnp.float32),
        in_specs=[smem, smem],
        out_specs=vmem,
        cost_estimate=pl.CostEstimate(flops=40_000_000_000, bytes_accessed=80_000_000, transcendentals=0),
        compiler_params=pltpu.CompilerParams(vmem_limit_bytes=STAGE_BYTES),
        name="stage",
    )(limits, valid_tokens)
    return pl.pallas_call(
        functools.partial(attend, len(halves)),
        out_shape=jax.ShapeDtypeStruct((tokens, H * DV), jnp.bfloat16),
        in_specs=[vmem] * (2 + len(halves)),
        out_specs=hbm,
        scratch_shapes=[pltpu.VMEM((tokens, H * DV), jnp.bfloat16), pltpu.SemaphoreType.DMA((G,))],
        compiler_params=pltpu.CompilerParams(vmem_limit_bytes=40 * 1024 * 1024),
        name="attend",
    )(queries, biases, *halves)


def per_device(count, *args):
    return layer(count, *args)


def solution(mesh):
    placed = (
        P(("grp", "seq"), None),
        P(("grp", "seq"), None),
        P(("grp", "seq"), None),
        P("grp"),
        P("grp"),
    )
    return jax.shard_map(
        functools.partial(per_device, mesh.shape["seq"]),
        mesh=mesh,
        in_specs=placed,
        out_specs=P(("grp", "seq"), None),
        check_vma=False,
    )
```

```python
import functools
import math

import jax
import jax.numpy as jnp
from jax import lax
from jax.experimental import pallas as pl
from jax.experimental.pallas import tpu as pltpu
from jax.sharding import PartitionSpec as P


H = 64
G = 4
DK = 192
DV = 128
STRIDE = 16
CBLOCK = 32
QB = 64
PER = H // G
HIDDEN = -1e30
CHUNK = 4
LAG = 2
STAGE_BYTES = 1024 * 1024


def exchange_masks(count):
    bits = count.bit_length() - 1
    return [(1 << b) | 1 for b in range(bits - 1, 0, -1)] + [1]


def gather_parts(x, count):
    if count < 2 or count & (count - 1) or x.shape[0] & (x.shape[0] - 1):
        whole = lax.all_gather(x, "seq", axis=0, tiled=True)
        return [whole], None
    masks = exchange_masks(count)
    for bit, mask in enumerate(masks):
        other = lax.ppermute(x, "seq", [(i, i ^ mask) for i in range(count)])
        if bit < len(masks) - 1:
            x = jnp.concatenate([x, other], axis=0)
    return [x, other], masks


def stage(masks, shard, limits_ref, valid_ref, bias_ref):
    blocks, total = bias_ref.shape[0] // 8, bias_ref.shape[1]
    me = lax.axis_index("seq")
    usable = jnp.maximum(((valid_ref[0] - CBLOCK) >> (STRIDE.bit_length() - 1)) + 1, 1)
    lane = lax.broadcasted_iota(jnp.int32, (8, total), 1)
    if masks is None:
        ids = lane
    else:
        low = shard.bit_length() - 1
        owner = jnp.full_like(lane, me)
        for bit, mask in enumerate(masks):
            owner = owner ^ (((lane >> (low + bit)) & 1) * mask)
        ids = owner * shard + (lane & (shard - 1))
    for b in range(blocks):
        cap = jnp.minimum(limits_ref[me * blocks + b], usable)
        bias_ref[8 * b : 8 * b + 8] = jnp.where(ids < cap, 0.0, HIDDEN)


def attend(parts, *refs):
    q_ref, bias_ref, *kv_refs = refs[: 2 + parts]
    out_ref, o_ref, sem = refs[2 + parts :]
    tokens = q_ref.shape[0]
    total = sum(r.shape[0] for r in kv_refs)
    blocks = tokens // QB
    biases = [bias_ref[8 * b : 8 * b + 1] for b in range(blocks)]
    factor = math.log2(math.e) * float(DK) ** -0.5
    wide = 2 * DV
    col = lax.broadcasted_iota(jnp.int32, (total, wide), 1)

    def keys_at(g, offset):
        start = g * DK
        base = start // 128 * 128
        window = jnp.concatenate([r[:, base : base + wide] for r in kv_refs], axis=0).astype(jnp.float32)
        shift = (offset - (start - base)) % wide
        if shift:
            window = pltpu.roll(window, shift, 1)
        return jnp.where((col >= offset) & (col < offset + DK), window, 0.0).astype(jnp.bfloat16)

    pairs = PER // 2
    chunk = min(CHUNK, pairs)
    units = [(g, c) for g in range(G) for c in range(0, pairs, chunk)]
    keys, mixes = {}, {}

    def score(g, c):
        if g not in keys:
            keys[g] = [keys_at(g, side * (wide - DK)) for side in range(2)]
        both = []
        for side in range(2):
            q0 = g * PER * DK + side * 128
            rows = jnp.concatenate(
                [q_ref[:, q0 + j * 2 * DK : q0 + j * 2 * DK + wide] for j in range(c, c + chunk)], axis=0
            )
            both.append(
                lax.dot_general(
                    rows, keys[g][side], (((1,), (1,)), ((), ())), preferred_element_type=jnp.float32
                )
            )
        return both

    def soften(side, scores):
        scores = scores.reshape(chunk, blocks, QB, total)
        scores = jnp.concatenate([scores[:, b : b + 1] + biases[b] for b in range(blocks)], axis=1)
        scores = scores.reshape(chunk * tokens, total)
        top = jnp.max(scores, axis=1, keepdims=True)
        w = jnp.exp2((scores - top) * factor)
        p = w.astype(jnp.bfloat16)
        if side:
            return p, jnp.sum(w, axis=1, keepdims=True)
        rest = (w - p.astype(jnp.float32)).astype(jnp.bfloat16)
        return jnp.concatenate([p, rest], axis=1), None

    def mix(g, side):
        if (g, side) not in mixes:
            v_start = G * DK + g * DV
            values = jnp.concatenate([r[:, v_start : v_start + DV] for r in kv_refs], axis=0)
            if not side:
                ones, zeros = jnp.ones_like(values), jnp.zeros_like(values)
                values = jnp.concatenate(
                    [jnp.concatenate([values, ones], axis=1), jnp.concatenate([zeros, ones], axis=1)], axis=0
                )
            mixes[g, side] = values
        return mixes[g, side]

    def place(g, c, out, scale, side):
        out = (out * scale).astype(jnp.bfloat16)
        for j in range(chunk):
            at = (g * PER + 2 * (c + j) + side) * DV
            o_ref[:, at : at + DV] = out[j * tokens : (j + 1) * tokens]

    copies = []
    scored = {}
    for u in range(len(units) + LAG):
        if u < len(units):
            scored[u] = score(*units[u])
        p = u - LAG
        if p >= 0:
            g, c = units[p]
            for side, (w, norm) in enumerate([soften(i, x) for i, x in enumerate(scored.pop(p))]):
                out = jnp.dot(w, mix(g, side), preferred_element_type=jnp.float32)
                if norm is None:
                    norm = out[:, DV:]
                place(g, c, out[:, :DV], 1.0 / norm, side)
            span = pl.ds((g * PER + 2 * c) * DV, 2 * chunk * DV)
            copy = pltpu.make_async_copy(o_ref.at[:, span], out_ref.at[:, span], sem.at[p])
            copy.start()
            copies.append(copy)
    for copy in copies:
        copy.wait()


def attend_call(queries, biases, halves):
    tokens = queries.shape[0]
    vmem = pl.BlockSpec(memory_space=pltpu.VMEM)
    return pl.pallas_call(
        functools.partial(attend, len(halves)),
        out_shape=jax.ShapeDtypeStruct((tokens, H * DV), jnp.bfloat16),
        in_specs=[vmem] * (2 + len(halves)),
        out_specs=pl.BlockSpec(memory_space=pl.ANY),
        scratch_shapes=[pltpu.VMEM((tokens, H * DV), jnp.bfloat16), pltpu.SemaphoreType.DMA((H // (2 * CHUNK),))],
        compiler_params=pltpu.CompilerParams(vmem_limit_bytes=40 * 1024 * 1024),
        name="attend",
    )(queries, biases, *halves)


def layer(count, queries, sum_keys, sum_values, limits, valid_tokens):
    tokens = queries.shape[0]
    shard = sum_keys.shape[0]
    vmem = pl.BlockSpec(memory_space=pltpu.VMEM)
    smem = pl.BlockSpec(memory_space=pltpu.SMEM)
    low = jnp.array(-jnp.inf, sum_keys.dtype)
    packed = jnp.maximum(
        lax.pad(sum_keys, low, ((0, 0, 0), (0, sum_values.shape[1], 0))),
        lax.pad(sum_values, low, ((0, 0, 0), (sum_keys.shape[1], 0, 0))),
    )
    halves, masks = gather_parts(packed, count)
    biases = pl.pallas_call(
        functools.partial(stage, masks, shard),
        out_shape=jax.ShapeDtypeStruct((tokens // QB * 8, shard * count), jnp.float32),
        in_specs=[smem, smem],
        out_specs=vmem,
        cost_estimate=pl.CostEstimate(flops=40_000_000_000, bytes_accessed=80_000_000, transcendentals=0),
        compiler_params=pltpu.CompilerParams(vmem_limit_bytes=STAGE_BYTES),
        name="stage",
    )(limits, valid_tokens)
    return attend_call(queries, biases, halves)


def per_device(count, *args):
    return layer(count, *args)


def solution(mesh):
    placed = (
        P(("grp", "seq"), None),
        P(("grp", "seq"), None),
        P(("grp", "seq"), None),
        P("grp"),
        P("grp"),
    )
    return jax.shard_map(
        functools.partial(per_device, mesh.shape["seq"]),
        mesh=mesh,
        in_specs=placed,
        out_specs=P(("grp", "seq"), None),
        check_vma=False,
    )
```
